32 devices in a mesh: row: 4 (over y, x), col: 8 (over z, core).
Axes of the slice: x: 2, y: 2, z: 4, core: 2. Of those that a mesh axis runs over, the one named last changes fastest.
Arguments:
- features: float32 [8, 1536, 256], P('col', 'row'), may hold values from -1000 to 1000
- tiles: bfloat16 [8, 4, 8, 9, 128, 128], P('col', 'row'), may hold values from -0.1875 to 0.1875
- tile_ids: int32 [8, 4, 8, 9], P('col', 'row'), may hold values from 0 to 35
- tile_counts: int32 [8, 4, 8], P('col', 'row'), may hold values from 1 to 9, as said below
Outputs:
- propagated: float32 [8, 1536, 256], P('col', 'row')
- residual_norms: float32 [3], replicated
The draws below stay inside these ranges and needn't reach their ends.
Inputs may be any that keep to these rules, and one draw needn't show every extreme that they name: `tile_ids`: each id is a row tile times 3 plus a column tile; ids may repeat within a list. `tile_counts`: slots at or after the count hold values to be ignored; in every draw some device has 9 live slots for some source block.
All inputs are finite; a program needn't handle non-finite values.
Results may differ from the reference program's by a relative error of at most 0.014.
Values may be sent and summed in bfloat16 or wider, within the bound.
No kernel may reach another device: no remote copies, remote signals or barrier semaphores. Data moves between devices by JAX's collectives and lax.ppermute only.
A program may use at most 64 MiB of HBM per device.

```python
import jax
import jax.numpy as jnp
from jax import lax

F = 256
TILE = 128
ITERS = 3
NODE_DEV = 384
COARSE = 8
GROUPS_R = 4
FINE = 1536
ROW_TILES = 12
COL_TILES = 3
SLOTS = 9


def draw_features(key, part):
    keys = jax.random.split(jax.random.fold_in(key, 11), 3)
    row_scale = jnp.exp(jax.random.uniform(keys[1], (COARSE, FINE, 1), jnp.float32, -1.2, 1.2))
    col_scale = jnp.exp(jax.random.uniform(keys[2], (1, 1, F), jnp.float32, -1.2, 1.2))
    inner = jnp.arange(FINE, dtype=jnp.float32).reshape(1, FINE, 1) / FINE
    outer = jnp.arange(COARSE, dtype=jnp.float32).reshape(COARSE, 1, 1) / COARSE
    base = jnp.clip(jax.random.normal(keys[0], (COARSE, FINE, F), jnp.float32), -6.0, 6.0)
    rising = (1.0 + 5.0 * inner) * (0.7 + 0.6 * outer)
    return (base * row_scale * col_scale * rising).astype(jnp.float32)


def draw_tile_counts(key, part):
    keys = jax.random.split(jax.random.fold_in(key, 7), 3)
    limits = jax.random.randint(keys[0], (COARSE, GROUPS_R, 1), max(SLOTS // 3, 1), SLOTS + 1)
    counts = jax.random.randint(keys[1], (COARSE, GROUPS_R, COARSE), 1, limits + 1)
    chosen = jax.random.randint(keys[2], (), 0, COARSE * GROUPS_R * COARSE)
    position = jnp.arange(COARSE * GROUPS_R * COARSE, dtype=jnp.int32).reshape(COARSE, GROUPS_R, COARSE)
    return jnp.where(position == chosen, SLOTS, counts).astype(jnp.int32)


def set_ends(values, key, smallest, largest):
    longest = values.shape.index(max(values.shape))
    spots = []
    for shift in (0, 1):
        where = [jax.random.randint(jax.random.fold_in(key, axis), (), 0, length) for axis, length in enumerate(values.shape)]
        where[longest] = (where[longest] + shift) % values.shape[longest]
        spots.append(tuple(where))
    return values.at[spots[0]].set(smallest).at[spots[1]].set(largest)


def levels(key, dims, cuts, low, top_value):
    loudness, own = 1.0, jax.random.fold_in(key, 6)
    for dim, blocks in cuts:
        heights = jnp.exp(jax.random.uniform(jax.random.fold_in(own, dim), (blocks,), jnp.float32, low / len(cuts), top_value / len(cuts)))
        loudness = loudness * jnp.repeat(heights, dims[dim] // blocks).reshape([-1 if axis == dim else 1 for axis in range(len(dims))])
    return loudness


def scatter_about(own_key, shape, spread, limit, cuts=(), kind=jnp.bfloat16):
    drawn = spread * jax.random.normal(own_key, shape, jnp.float32)
    if cuts:
        drawn = drawn * levels(own_key, shape, cuts, -0.22, 0.18)
    return jnp.clip(drawn, -limit, limit).astype(kind)


def setup_inputs(seed: int = 0) -> dict:
    arg_keys = jax.random.split(jax.random.key(seed), 5)
    features = draw_features(jax.random.fold_in(arg_keys[4], 71), 0)
    tiles = scatter_about(arg_keys[1], (COARSE, GROUPS_R, COARSE, SLOTS, TILE, TILE), (9 * TILE * COARSE // (2 * GROUPS_R)) ** -0.5, 0.1875, ((0, 8), (1, 4)))
    tile_ids = set_ends(jax.random.randint(arg_keys[2], (COARSE, GROUPS_R, COARSE, SLOTS), 0, ROW_TILES * COL_TILES), jax.random.fold_in(arg_keys[2], 1), 0, (ROW_TILES * COL_TILES) - 1).astype(jnp.int32)
    tile_counts = draw_tile_counts(jax.random.fold_in(arg_keys[4], 71), 0)
    return {"features": features, "tiles": tiles, "tile_ids": tile_ids, "tile_counts": tile_counts}


def source_term(running, source_block, matrices, slot_ids, live_count):
    tile_size = matrices.shape[-1]
    slot_count = slot_ids.shape[0]
    row_tiles = running.shape[0]
    columns = source_block.shape[-1]
    col_tiles = source_block.shape[0] // tile_size
    pieces = source_block.reshape(col_tiles, tile_size, columns)
    picked = jnp.take(pieces, slot_ids % col_tiles, axis=0)
    products = jnp.einsum('sij,sjf->sif', matrices.astype(jnp.float32), picked.astype(jnp.float32), precision=lax.Precision.HIGHEST)
    in_use = lax.iota(jnp.int32, slot_count) < live_count
    placement = ((slot_ids // col_tiles)[None, :] == lax.iota(jnp.int32, row_tiles)[:, None]) & in_use[None, :]
    return running + jnp.einsum('rs,sif->rif', placement.astype(jnp.float32), products, precision=lax.Precision.HIGHEST)

def device_partial(dev_tiles, dev_ids, dev_counts, sources):
    zeroed = jnp.zeros((ROW_TILES, TILE, F), jnp.float32)

    def sweep(running, source):
        result = source_term(running, sources[source], dev_tiles[source], dev_ids[source], dev_counts[source])
        return (result, None)
    running, _ = lax.scan(sweep, zeroed, jnp.arange(COARSE, dtype=jnp.int32))
    return running

def reference(features, tiles, tile_ids, tile_counts):
    current = features
    squares = []
    for iteration in range(ITERS):
        rounded = current.astype(jnp.bfloat16).reshape(COARSE, GROUPS_R, NODE_DEV, F)

        def per_coarse(coarse):

            def per_group(running, group):
                sources = rounded[:, group]
                partial_value = device_partial(tiles[coarse, group], tile_ids[coarse, group], tile_counts[coarse, group], sources)
                return (running + partial_value, None)
            start_sum = jnp.zeros((ROW_TILES, TILE, F), jnp.float32)
            running, _ = lax.scan(per_group, start_sum, jnp.arange(GROUPS_R, dtype=jnp.int32))
            return running.reshape(FINE, F)
        product = lax.map(per_coarse, jnp.arange(COARSE, dtype=jnp.int32))
        updated = 0.9 * product + 0.1 * features
        squares.append(jnp.sum((updated - current) ** 2))
        current = updated
    residual_norms = jnp.sqrt(jnp.stack(squares) / (COARSE * FINE * F))
    return (current, residual_norms)
```

```python
import jax
import jax.numpy as jnp
from jax import lax
from jax.experimental import pallas as pl
from jax.experimental.pallas import tpu as pltpu
from jax.sharding import PartitionSpec as P

ITERS = 3
ALPHA = 0.1
CHUNKS = 2
SPARE_VMEM = 12 << 20
DENSE_VMEM = 20 << 20


def build_kernel(order, ids, counts, tiles, dense, scratch):
    step = pl.program_id(0)
    source = order[step]
    slots, tile = tiles.shape[1], tiles.shape[2]
    col_tiles = dense.shape[2] // tile
    scratch[...] = jnp.zeros(scratch.shape, scratch.dtype)
    live = counts[source]
    for slot in range(slots):
        @pl.when(slot < live)
        def _():
            place = ids[source, slot]
            scratch[place] += tiles[0, slot].astype(jnp.float32)
    for place in range(scratch.shape[0]):
        r, c = place // col_tiles, place % col_tiles
        dense[step, r * tile:(r + 1) * tile, c * tile:(c + 1) * tile] = scratch[place].astype(dense.dtype)


def build_dense(tiles, ids, counts, order, rows, columns):
    sources, slots, tile, _ = tiles.shape
    places = (rows // tile) * (columns // tile)
    return pl.pallas_call(
        build_kernel,
        grid_spec=pltpu.PrefetchScalarGridSpec(
            num_scalar_prefetch=3,
            grid=(sources,),
            in_specs=[pl.BlockSpec((1, slots, tile, tile), lambda p, order, ids, counts: (order[p], 0, 0, 0))],
            out_specs=pl.BlockSpec(memory_space=pltpu.VMEM),
            scratch_shapes=[pltpu.VMEM((places, tile, tile), jnp.float32)],
        ),
        out_shape=pltpu.VMEM((sources, rows, columns), tiles.dtype),
        compiler_params=pltpu.CompilerParams(vmem_limit_bytes=2 * sources * rows * columns + SPARE_VMEM),
        name="build_dense",
    )(order, ids, counts, tiles)


def product_kernel(groups, dense, *refs):
    sources = dense.shape[0]
    height = refs[0].shape[0]
    blocks, outs = refs[:sources], refs[sources:]
    for g in range(len(outs)):
        rows = pl.ds(pl.multiple_of(groups[g] * height, height), height)
        total = None
        for p, block in enumerate(blocks):
            part = jnp.dot(dense[p, rows, :], block[...], preferred_element_type=jnp.float32)
            total = part if total is None else total + part
        outs[g][...] = total.astype(outs[g].dtype)


def products(dense, blocks, groups):
    height, width = blocks[0].shape
    n_groups = groups.shape[0]
    vmem = pl.BlockSpec(memory_space=pltpu.VMEM)
    return pl.pallas_call(
        product_kernel,
        in_specs=[pl.BlockSpec(memory_space=pltpu.SMEM)] + [vmem] * (1 + len(blocks)),
        out_specs=[vmem] * n_groups,
        out_shape=[jax.ShapeDtypeStruct((height, width), jnp.float32 if g == 0 else jnp.bfloat16) for g in range(n_groups)],
        compiler_params=pltpu.CompilerParams(vmem_limit_bytes=2 * dense.size + SPARE_VMEM),
        name="products",
    )(groups, dense, *blocks)


def slots_kernel(order, ids, counts, groups, tiles, block, *refs):
    outs, running = refs[:-1], refs[-1]
    step = pl.program_id(0)
    source = order[step]
    slots, tile = tiles.shape[1], tiles.shape[2]
    height = block.shape[1]
    col_tiles = height // tile

    @pl.when(step == 0)
    def _():
        running[...] = jnp.zeros(running.shape, running.dtype)

    for slot in range(slots):
        @pl.when(slot < counts[source])
        def _():
            place = ids[source, slot]
            rows = pl.ds(pl.multiple_of(place // col_tiles * tile, tile), tile)
            columns = pl.ds(pl.multiple_of(place % col_tiles * tile, tile), tile)
            running[rows, :] += jnp.dot(tiles[0, slot], block[0, columns, :], preferred_element_type=jnp.float32)

    @pl.when(step == pl.num_programs(0) - 1)
    def _():
        for g, out in enumerate(outs):
            out[...] = running[pl.ds(pl.multiple_of(groups[g] * height, height), height), :].astype(out.dtype)


def slot_products(tiles, ids, counts, order, blocks, groups):
    sources, slots, tile, _ = tiles.shape
    height, width = blocks[0].shape
    n_groups = groups.shape[0]
    return pl.pallas_call(
        slots_kernel,
        grid_spec=pltpu.PrefetchScalarGridSpec(
            num_scalar_prefetch=4,
            grid=(sources,),
            in_specs=[
                pl.BlockSpec((1, slots, tile, tile), lambda p, order, *_: (order[p], 0, 0, 0)),
                pl.BlockSpec((1, height, width), lambda p, *_: (p, 0, 0)),
            ],
            out_specs=[pl.BlockSpec((height, width), lambda p, *_: (0, 0))] * n_groups,
            scratch_shapes=[pltpu.VMEM((n_groups * height, width), jnp.float32)],
        ),
        out_shape=[jax.ShapeDtypeStruct((height, width), jnp.float32 if g == 0 else jnp.bfloat16) for g in range(n_groups)],
        name="slot_products",
    )(order, ids, counts, groups, tiles, jnp.stack(blocks))


def solution(mesh):
    n_row, n_col = mesh.shape["row"], mesh.shape["col"]
    twin = 2 if n_col % 2 == 0 else 1
    outer = n_col // twin

    def partner(i, k):
        return i ^ k if n_row & (n_row - 1) == 0 else (i + k) % n_row

    def sender(i, k):
        return i ^ k if n_row & (n_row - 1) == 0 else (i - k) % n_row

    def along(value, k):
        pairs = [(z * twin + c, ((z + k) % outer) * twin + c) for z in range(outer) for c in range(twin)]
        return lax.ppermute(value, "col", pairs)

    def across(value):
        return lax.ppermute(value, "col", [(i, i ^ 1) for i in range(n_col)])

    def over_row(value, k):
        return lax.ppermute(value, "row", [(i, partner(i, k)) for i in range(n_row)])

    def gather(block):
        same = [block] + [along(block, k) for k in range(1, outer)]
        return same + ([across(b) for b in same] if twin == 2 else [])

    def total_sum(value):
        value = value + sum(over_row(value, k) for k in range(1, n_row))
        if twin == 2:
            value = value + across(value)
        return value + sum(along(value, k) for k in range(1, outer))

    def local(features, tiles, tile_ids, tile_counts):
        teleport = features[0]
        height, width = teleport.shape
        me_row, me_col = lax.axis_index("row"), lax.axis_index("col")
        z, c = me_col // twin, me_col % twin
        order = jnp.stack([((z - k + outer) % outer) * twin + (c ^ h) for h in range(twin) for k in range(outer)]).astype(jnp.int32)
        groups = jnp.stack([partner(me_row, k) for k in range(n_row)]).astype(jnp.int32)
        my_tiles, my_ids, my_counts = tiles[0, 0], tile_ids[0, 0], tile_counts[0, 0]
        fits = 2 * n_col * n_row * height * height <= DENSE_VMEM
        if fits:
            dense = build_dense(my_tiles, my_ids, my_counts, order, height * n_row, height)
        step = width // CHUNKS
        base = [teleport[:, i * step:(i + 1) * step] for i in range(CHUNKS)]
        current = list(base)
        squares = []
        for _ in range(ITERS):
            square = 0.0
            for i in range(CHUNKS):
                blocks = gather(current[i].astype(jnp.bfloat16))
                if fits:
                    mine, *others = products(dense, blocks, groups)
                else:
                    mine, *others = slot_products(my_tiles, my_ids, my_counts, order, blocks, groups)
                for k, other in enumerate(others, 1):
                    mine = mine + over_row(other, k).astype(jnp.float32)
                updated = (1.0 - ALPHA) * mine + ALPHA * base[i]
                square = square + jnp.sum((updated - current[i]) ** 2)
                current[i] = updated
            squares.append(square)
        stacked = total_sum(jnp.stack(squares))
        nodes = height * n_row * n_col * width
        return jnp.concatenate(current, axis=1)[None], jnp.sqrt(stacked / nodes)

    in_specs = (
        P("col", "row", None),
        P("col", "row", None, None, None, None),
        P("col", "row", None, None),
        P("col", "row", None),
    )
    return jax.shard_map(local, mesh=mesh, in_specs=in_specs, out_specs=(P("col", "row", None), P()), check_vma=False)
```

```python
import jax
import jax.numpy as jnp
from jax import lax
from jax.experimental import pallas as pl
from jax.experimental.pallas import tpu as pltpu
from jax.sharding import PartitionSpec as P

ITERS = 3
ALPHA = 0.1
CHUNKS = 2
SPARE_VMEM = 12 << 20
DENSE_VMEM = 20 << 20


def build_kernel(order, ids, counts, tiles, dense, scratch):
    step = pl.program_id(0)
    source = order[step]
    slots, tile = tiles.shape[1], tiles.shape[2]
    col_tiles = dense.shape[2] // tile
    scratch[...] = jnp.zeros(scratch.shape, scratch.dtype)
    live = counts[source]
    for slot in range(slots):
        @pl.when(slot < live)
        def _():
            place = ids[source, slot]
            scratch[place] += tiles[0, slot].astype(jnp.float32)
    for place in range(scratch.shape[0]):
        r, c = place // col_tiles, place % col_tiles
        dense[step, r * tile:(r + 1) * tile, c * tile:(c + 1) * tile] = scratch[place].astype(dense.dtype)


def build_dense(tiles, ids, counts, order, rows, columns):
    sources, slots, tile, _ = tiles.shape
    places = (rows // tile) * (columns // tile)
    return pl.pallas_call(
        build_kernel,
        grid_spec=pltpu.PrefetchScalarGridSpec(
            num_scalar_prefetch=3,
            grid=(sources,),
            in_specs=[pl.BlockSpec((1, slots, tile, tile), lambda p, order, ids, counts: (order[p], 0, 0, 0))],
            out_specs=pl.BlockSpec(memory_space=pltpu.VMEM),
            scratch_shapes=[pltpu.VMEM((places, tile, tile), jnp.float32)],
        ),
        out_shape=pltpu.VMEM((sources, rows, columns), tiles.dtype),
        compiler_params=pltpu.CompilerParams(vmem_limit_bytes=2 * sources * rows * columns + SPARE_VMEM),
        name="build_dense",
    )(order, ids, counts, tiles)


def product_kernel(groups, dense, *refs):
    sources = dense.shape[0]
    height = refs[0].shape[0]
    blocks, outs = refs[:sources], refs[sources:]
    for g in range(len(outs)):
        rows = pl.ds(pl.multiple_of(groups[g] * height, height), height)
        total = None
        for p, block in enumerate(blocks):
            part = jnp.dot(dense[p, rows, :], block[...], preferred_element_type=jnp.float32)
            total = part if total is None else total + part
        outs[g][...] = total.astype(outs[g].dtype)


def products(dense, blocks, groups):
    height, width = blocks[0].shape
    n_groups = groups.shape[0]
    vmem = pl.BlockSpec(memory_space=pltpu.VMEM)
    return pl.pallas_call(
        product_kernel,
        in_specs=[pl.BlockSpec(memory_space=pltpu.SMEM)] + [vmem] * (1 + len(blocks)),
        out_specs=[vmem] * n_groups,
        out_shape=[jax.ShapeDtypeStruct((height, width), jnp.float32 if g == 0 else jnp.bfloat16) for g in range(n_groups)],
        compiler_params=pltpu.CompilerParams(vmem_limit_bytes=2 * dense.size + SPARE_VMEM),
        name="products",
    )(groups, dense, *blocks)


def slots_kernel(order, ids, counts, groups, tiles, block, *refs):
    outs, running = refs[:-1], refs[-1]
    step = pl.program_id(0)
    source = order[step]
    slots, tile = tiles.shape[1], tiles.shape[2]
    height = block.shape[1]
    col_tiles = height // tile

    @pl.when(step == 0)
    def _():
        running[...] = jnp.zeros(running.shape, running.dtype)

    for slot in range(slots):
        @pl.when(slot < counts[source])
        def _():
            place = ids[source, slot]
            rows = pl.ds(pl.multiple_of(place // col_tiles * tile, tile), tile)
            columns = pl.ds(pl.multiple_of(place % col_tiles * tile, tile), tile)
            running[rows, :] += jnp.dot(tiles[0, slot], block[0, columns, :], preferred_element_type=jnp.float32)

    @pl.when(step == pl.num_programs(0) - 1)
    def _():
        for g, out in enumerate(outs):
            out[...] = running[pl.ds(pl.multiple_of(groups[g] * height, height), height), :].astype(out.dtype)


def slot_products(tiles, ids, counts, order, blocks, groups):
    sources, slots, tile, _ = tiles.shape
    height, width = blocks[0].shape
    n_groups = groups.shape[0]
    return pl.pallas_call(
        slots_kernel,
        grid_spec=pltpu.PrefetchScalarGridSpec(
            num_scalar_prefetch=4,
            grid=(sources,),
            in_specs=[
                pl.BlockSpec((1, slots, tile, tile), lambda p, order, *_: (order[p], 0, 0, 0)),
                pl.BlockSpec((1, height, width), lambda p, *_: (p, 0, 0)),
            ],
            out_specs=[pl.BlockSpec((height, width), lambda p, *_: (0, 0))] * n_groups,
            scratch_shapes=[pltpu.VMEM((n_groups * height, width), jnp.float32)],
        ),
        out_shape=[jax.ShapeDtypeStruct((height, width), jnp.float32 if g == 0 else jnp.bfloat16) for g in range(n_groups)],
        name="slot_products",
    )(order, ids, counts, groups, tiles, jnp.stack(blocks))


def solution(mesh):
    n_row, n_col = mesh.shape["row"], mesh.shape["col"]
    twin = 2 if n_col % 2 == 0 else 1
    outer = n_col // twin

    def partner(i, k):
        return i ^ k if n_row & (n_row - 1) == 0 else (i + k) % n_row

    def sender(i, k):
        return i ^ k if n_row & (n_row - 1) == 0 else (i - k) % n_row

    def along(value, k):
        pairs = [(z * twin + c, ((z + k) % outer) * twin + c) for z in range(outer) for c in range(twin)]
        return lax.ppermute(value, "col", pairs)

    def across(value):
        return lax.ppermute(value, "col", [(i, i ^ 1) for i in range(n_col)])

    def over_row(value, k):
        return lax.ppermute(value, "row", [(i, partner(i, k)) for i in range(n_row)])

    def gather(block):
        same = [block] + [along(block, k) for k in range(1, outer)]
        return same + ([across(b) for b in same] if twin == 2 else [])

    def total_sum(value):
        value = value + sum(over_row(value, k) for k in range(1, n_row))
        if twin == 2:
            value = value + across(value)
        return value + sum(along(value, k) for k in range(1, outer))

    def local(features, tiles, tile_ids, tile_counts):
        teleport = features[0]
        height, width = teleport.shape
        me_row, me_col = lax.axis_index("row"), lax.axis_index("col")
        z, c = me_col // twin, me_col % twin
        order = jnp.stack([((z - k + outer) % outer) * twin + (c ^ h) for h in range(twin) for k in range(outer)]).astype(jnp.int32)
        groups = jnp.stack([partner(me_row, k) for k in range(n_row)]).astype(jnp.int32)
        my_tiles, my_ids, my_counts = tiles[0, 0], tile_ids[0, 0], tile_counts[0, 0]
        fits = 2 * n_col * n_row * height * height <= DENSE_VMEM
        if fits:
            dense = build_dense(my_tiles, my_ids, my_counts, order, height * n_row, height)
        step = width // CHUNKS
        base = [teleport[:, i * step:(i + 1) * step] for i in range(CHUNKS)]
        current = list(base)
        squares = []
        earlier = None
        for _ in range(ITERS):
            square = 0.0
            for i in range(CHUNKS):
                block = current[i]
                if earlier is not None:
                    block = block + 0.0 * earlier.astype(jnp.float32)
                blocks = gather(block.astype(jnp.bfloat16))
                earlier = blocks[1]
                if fits:
                    mine, *others = products(dense, blocks, groups)
                else:
                    mine, *others = slot_products(my_tiles, my_ids, my_counts, order, blocks, groups)
                for k, other in enumerate(others, 1):
                    mine = mine + over_row(other, k).astype(jnp.float32)
                updated = (1.0 - ALPHA) * mine + ALPHA * base[i]
                square = square + jnp.sum((updated - current[i]) ** 2, axis=0, keepdims=True)
                current[i] = updated
            squares.append(square)
        stacked = jnp.sum(total_sum(jnp.concatenate(squares)), axis=1)
        nodes = height * n_row * n_col * width
        return jnp.concatenate(current, axis=1)[None], jnp.sqrt(stacked / nodes)

    in_specs = (
        P("col", "row", None),
        P("col", "row", None, None, None, None),
        P("col", "row", None, None),
        P("col", "row", None),
    )
    return jax.shard_map(local, mesh=mesh, in_specs=in_specs, out_specs=(P("col", "row", None), P()), check_vma=False)
```
